32 devices in a mesh: group: 2 (over y), win: 16 (over z, x, core).
Axes of the slice: x: 2, y: 2, z: 4, core: 2. Of those that a mesh axis runs over, the one named last changes fastest.
Arguments:
- img_qkv: bfloat16 [64, 256, 4608], P(('group', 'win')), parts along dimension 0, may hold values from -100 to 100
- txt_kv: bfloat16 [64, 128, 3072], P(('group', 'win')), parts along dimension 0, may hold values from -6 to 6
- hidden: bfloat16 [64, 256, 3072], P(('group', 'win')), parts along dimension 0, may hold values from -6 to 6
- w_proj: bfloat16 [1536, 3072], P('win'), may hold values from -0.15625 to 0.15625
- w_out: bfloat16 [3072, 64], replicated, may hold values from -0.109375 to 0.109375
- modulation: float32 [6, 3072], P('group'), parts along dimension 0, may hold values from -3 to 3
- anchors: int32 [64, 2], P(('group', 'win')), parts along dimension 0, may hold values from 0 to 255, as said below
- blend_weight: int32 [64, 32, 32], P(('group', 'win')), parts along dimension 0, may hold values from 0 to 8
Outputs:
- velocity: float32 [16, 512, 64], P(None, ('group', 'win')), parts along dimension 1
The draws below stay inside these ranges and needn't reach their ends.
There are 2 independent parts, one for each index of `group`. The reference program is written for one: setup_inputs(seed, part) draws one part's arguments, and reference() takes and returns one part's arrays. A program takes and returns all parts, laid end to end along the dimension named above; an argument that names none is the same for every part. Nothing has to cross between parts.
Inputs may be any that keep to these rules, and one draw needn't show every extreme that they name: `anchors`: window w's anchor row lies in [16 * (w // 2), 16 * (w // 2) + 16); its columns wrap around the panorama; the 2 windows w with the same w // 2 have anchor columns (s + 32 * (w % 2)) mod 64 for one s of that band, so that they cover all 64 columns.
All inputs are finite; a program needn't handle non-finite values.
Results may differ from the reference program's by a relative error of at most 0.0029.
Values may be sent and summed in bfloat16 or wider, within the bound.
A program may use at most 128 MiB of HBM per device.

```python
import math
import jax
import jax.numpy as jnp
from jax import lax

D = 3072
HD = 128
C = 16
HEADS = 12
PATCH = 2
WIN = 32
TXT = 128
WIN_DEV = 2
LW = 64
BAND = 16
GRID = 16
P_SIZE = 256
HW = 1536
WINDOWS = 32
LH = 256


def draw_img_qkv(key, part):
    key_main = jax.random.fold_in(key, 11)
    values_all = jax.random.normal(key_main, (WINDOWS, P_SIZE, 3 * HW), jnp.float32)
    values_all = jnp.clip(values_all, -4.5, 4.5)
    return values_all.astype(jnp.bfloat16)


def draw_anchors(key, part):
    key_rows = jax.random.fold_in(key, 21)
    key_cols = jax.random.fold_in(key, 22)
    slot_index = jnp.arange(WINDOWS, dtype=jnp.int32)
    band_index = slot_index // WIN_DEV
    within = slot_index % WIN_DEV
    row_anchor = band_index * BAND + jax.random.randint(key_rows, (WINDOWS,), 0, BAND, jnp.int32)
    shift_all = jax.random.randint(key_cols, (WINDOWS,), 0, LW, jnp.int32)
    band_shift = shift_all[band_index * WIN_DEV]
    col_anchor = (band_shift + WIN * within) % LW
    return jnp.stack([row_anchor, col_anchor], axis=1).astype(jnp.int32)


def place_ends(values, rng, least, high):
    longest = values.shape.index(max(values.shape))
    spots = []
    for shift in (0, 1):
        where = [jax.random.randint(jax.random.fold_in(rng, axis), (), 0, length) for axis, length in enumerate(values.shape)]
        where[longest] = (where[longest] + shift) % values.shape[longest]
        spots.append(tuple(where))
    return values.at[spots[0]].set(least).at[spots[1]].set(high)


def block_levels(key, extent, shards, smallest, high):
    factor_of, own = 1.0, jax.random.fold_in(key, 6)
    for dim, parts in shards:
        heights = jnp.exp(jax.random.uniform(jax.random.fold_in(own, dim), (parts,), jnp.float32, smallest / len(shards), high / len(shards)))
        factor_of = factor_of * jnp.repeat(heights, extent[dim] // parts).reshape([-1 if axis == dim else 1 for axis in range(len(extent))])
    return factor_of


def scatter_about(stream_key, shape, scale, reach, shards=(), held_as=jnp.bfloat16):
    loudness = block_levels(stream_key, shape, shards, -0.22, 0.18) if shards else 1.0
    values = jax.random.normal(stream_key, shape, jnp.float32) * scale * loudness
    return jnp.minimum(jnp.maximum(values, -reach), reach).astype(held_as)


def setup_inputs(seed: int = 0, part: int = 0) -> dict:
    streams_of = jax.random.split(jax.random.key(seed), 9)
    own_keys = jax.random.split(jax.random.fold_in(streams_of[8], part), 9)
    return {
        "img_qkv": draw_img_qkv(jax.random.fold_in(jax.random.fold_in(streams_of[8], part), 71), part),
        "txt_kv": scatter_about(own_keys[1], (WINDOWS, TXT, 2 * HW), 1.0, 6.0, ((0, 16),)),
        "hidden": scatter_about(own_keys[2], (WINDOWS, P_SIZE, D), 1.0, 6.0, ((0, 16),)),
        "w_proj": scatter_about(streams_of[3], (HW, D), HW ** -0.5, 0.15625, ((0, 16),)),
        "w_out": scatter_about(streams_of[4], (D, C * PATCH * PATCH), D ** -0.5, 0.109375),
        "modulation": scatter_about(own_keys[5], (3, D), 0.5, 3.0, (), jnp.float32),
        "anchors": draw_anchors(jax.random.fold_in(jax.random.fold_in(streams_of[8], part), 71), part),
        "blend_weight": place_ends(jax.random.randint(own_keys[7], (WINDOWS, WIN, WIN), 0, 9), jax.random.fold_in(own_keys[7], 1), 0, 8).astype(jnp.int32),
    }


def window_velocity(one_qkv, one_txt, one_hidden, w_proj, w_out, modulation):
    features = HEADS * HD
    queries = one_qkv[:, :features].reshape(P_SIZE, HEADS, HD).astype(jnp.float32)
    all_keys = jnp.concatenate([one_txt[:, :features], one_qkv[:, features:2 * features]], axis=0)
    all_keys = all_keys.reshape(TXT + P_SIZE, HEADS, HD).astype(jnp.float32)
    all_values = jnp.concatenate([one_txt[:, features:], one_qkv[:, 2 * features:]], axis=0)
    all_values = all_values.reshape(TXT + P_SIZE, HEADS, HD).astype(jnp.float32)
    scores = jnp.einsum('qhd,khd->hqk', queries, all_keys) / math.sqrt(HD)
    scores = scores - lax.optimization_barrier(jnp.max(scores, axis=-1, keepdims=True))
    exp_scores = jnp.exp(scores)
    soft_weights = (exp_scores / lax.optimization_barrier(jnp.sum(exp_scores, axis=-1, keepdims=True))).astype(jnp.bfloat16)
    attended = jnp.einsum('hqk,khd->qhd', soft_weights.astype(jnp.float32), all_values)
    attended = attended.reshape(P_SIZE, features).astype(jnp.bfloat16)
    projected = jnp.dot(attended, w_proj, preferred_element_type=jnp.float32)
    residual = one_hidden.astype(jnp.float32) + modulation[0] * projected
    row_mean = lax.optimization_barrier(jnp.mean(residual, axis=-1, keepdims=True))
    centred = residual - row_mean
    row_var = lax.optimization_barrier(jnp.mean(centred * centred, axis=-1, keepdims=True))
    normed = centred * lax.rsqrt(row_var + 1e-06)
    modulated = (normed * (1.0 + modulation[1]) + modulation[2]).astype(jnp.bfloat16)
    return jnp.dot(modulated, w_out, preferred_element_type=jnp.float32)

def unpatch(patch_vel):
    window_count = patch_vel.shape[0]
    patch_grid = patch_vel.reshape(window_count, GRID, GRID, C, PATCH, PATCH)
    return patch_grid.transpose(0, 3, 1, 4, 2, 5).reshape(window_count, C, WIN, WIN)

def place_window(canvas, totals, contrib, weights, row_at, col_at):
    zero_index = jnp.zeros((), jnp.int32)
    region = lax.dynamic_slice(canvas, (zero_index, row_at, col_at), (C, WIN, WIN))
    canvas = lax.dynamic_update_slice(canvas, region + contrib, (zero_index, row_at, col_at))
    weight_region = lax.dynamic_slice(totals, (row_at, col_at), (WIN, WIN))
    totals = lax.dynamic_update_slice(totals, weight_region + weights, (row_at, col_at))
    return (canvas, totals)

def fold_columns(field):
    span_cols = field.shape[-1] - WIN
    leading = field[..., :span_cols]
    wrapped = field[..., span_cols:]
    padding = [(0, 0)] * (field.ndim - 1) + [(0, span_cols - WIN)]
    return leading + jnp.pad(wrapped, padding)

def reference(img_qkv, txt_kv, hidden, w_proj, w_out, modulation, anchors, blend_weight):

    def per_window(window_items):
        return window_velocity(window_items[0], window_items[1], window_items[2], w_proj, w_out, modulation)
    patch_vel = lax.map(per_window, (img_qkv, txt_kv, hidden))
    window_vel = unpatch(patch_vel)
    weights = blend_weight.astype(jnp.float32)
    contrib = window_vel * weights[:, None]
    canvas = jnp.zeros((C, LH + WIN, LW + WIN), jnp.float32)
    totals = jnp.zeros((LH + WIN, LW + WIN), jnp.float32)

    def add_one(window, running):
        row_at = anchors[window, 0].astype(jnp.int32)
        col_at = anchors[window, 1].astype(jnp.int32)
        return place_window(running[0], running[1], contrib[window], weights[window], row_at, col_at)
    canvas, totals = lax.fori_loop(0, WINDOWS, add_one, (canvas, totals))
    canvas = fold_columns(canvas)[:, :LH]
    totals = fold_columns(totals)[:LH]
    return canvas / jnp.maximum(totals, 1.0)[None]
```

```python
import functools
import math

import jax
import jax.numpy as jnp
from jax import lax
from jax.experimental import pallas as pl
from jax.experimental.pallas import tpu as pltpu
from jax.sharding import PartitionSpec as P

HD = 128
C = 16
HEADS = 12
PATCH = 2
WIN = 32
LW = 64
BAND = 16
GRID = 16


def shifted(block, axis, distance):
    devices = range(lax.axis_size(axis))
    route = [(i - distance, i) for i in devices if i - distance in devices]
    return lax.ppermute(block, axis, route)


def place_window(canvas, totals, contrib, weights, row_at, col_at):
    zero_index = jnp.zeros((), jnp.int32)
    region = lax.dynamic_slice(canvas, (zero_index, row_at, col_at), (C, WIN, WIN))
    canvas = lax.dynamic_update_slice(canvas, region + contrib, (zero_index, row_at, col_at))
    weight_region = lax.dynamic_slice(totals, (row_at, col_at), (WIN, WIN))
    totals = lax.dynamic_update_slice(totals, weight_region + weights, (row_at, col_at))
    return (canvas, totals)


def fold_columns(field):
    span_cols = field.shape[-1] - WIN
    leading = field[..., :span_cols]
    wrapped = field[..., span_cols:]
    padding = [(0, 0)] * (field.ndim - 1) + [(0, span_cols - WIN)]
    return leading + jnp.pad(wrapped, padding)


def plain_shards(img_qkv, txt_kv, hidden, w_proj, w_out, modulation, anchors, blend_weight):
    window_count, tokens, _ = img_qkv.shape
    features = HEADS * HD
    queries = img_qkv[:, :, :features].reshape(window_count, tokens, HEADS, HD)
    all_keys = jnp.concatenate(
        [txt_kv[:, :, :features], img_qkv[:, :, features : 2 * features]], axis=1
    )
    all_keys = all_keys.reshape(window_count, -1, HEADS, HD)
    all_values = jnp.concatenate([txt_kv[:, :, features:], img_qkv[:, :, 2 * features :]], axis=1)
    all_values = all_values.reshape(window_count, -1, HEADS, HD)
    scores = jnp.einsum(
        "wqhd,wkhd->whqk", queries, all_keys, preferred_element_type=jnp.float32
    ) / math.sqrt(HD)
    scores = scores - jnp.max(scores, axis=-1, keepdims=True)
    exp_scores = jnp.exp(scores)
    soft_weights = (exp_scores / jnp.sum(exp_scores, axis=-1, keepdims=True)).astype(jnp.bfloat16)
    attended = jnp.einsum(
        "whqk,wkhd->wqhd", soft_weights, all_values, preferred_element_type=jnp.float32
    )
    attended = attended.reshape(window_count * tokens, features).astype(jnp.bfloat16)
    whole_proj = lax.all_gather(w_proj, "win", axis=0, tiled=True)
    projected = jnp.dot(attended, whole_proj, preferred_element_type=jnp.float32)
    residual = (
        hidden.reshape(window_count * tokens, -1).astype(jnp.float32) + modulation[0] * projected
    )
    row_mean = jnp.mean(residual, axis=-1, keepdims=True)
    centred = residual - row_mean
    row_var = jnp.mean(centred * centred, axis=-1, keepdims=True)
    normed = centred * lax.rsqrt(row_var + 1e-06)
    modulated = (normed * (1.0 + modulation[1]) + modulation[2]).astype(jnp.bfloat16)
    patch_vel = jnp.dot(modulated, w_out, preferred_element_type=jnp.float32)
    patch_grid = patch_vel.reshape(window_count, GRID, GRID, C, PATCH, PATCH)
    window_vel = patch_grid.transpose(0, 3, 1, 4, 2, 5).reshape(window_count, C, WIN, WIN)
    weights = blend_weight.astype(jnp.float32)
    contrib = window_vel * weights[:, None]
    band_start = lax.axis_index("win") * BAND
    canvas = jnp.zeros((C, BAND + WIN, LW + WIN), jnp.float32)
    totals = jnp.zeros((BAND + WIN, LW + WIN), jnp.float32)

    def add_one(window, running):
        row_at = anchors[window, 0] - band_start
        col_at = anchors[window, 1]
        return place_window(
            running[0], running[1], contrib[window], weights[window], row_at, col_at
        )

    canvas, totals = lax.fori_loop(0, window_count, add_one, (canvas, totals))
    canvas = fold_columns(canvas)
    totals = fold_columns(totals)
    own_canvas = canvas[:, :BAND]
    own_totals = totals[:BAND]
    near_canvas = canvas[:, BAND : 2 * BAND]
    near_totals = totals[BAND : 2 * BAND]
    far_canvas = canvas[:, 2 * BAND :]
    far_totals = totals[2 * BAND :]
    prev_canvas, prev_totals = shifted((near_canvas, near_totals), "win", 1)
    second_canvas, second_totals = shifted((far_canvas, far_totals), "win", 2)
    sum_canvas = own_canvas + prev_canvas + second_canvas
    sum_totals = own_totals + prev_totals + second_totals
    return sum_canvas / jnp.maximum(sum_totals, 1.0)[None]


LOG2E = 1.4426950408889634
MESH_ID = pl.DeviceIdType.MESH


def block_kernel(
    n,
    qkv_hbm,
    txt_hbm,
    hid_hbm,
    wp_hbm,
    wout_ref,
    mod_ref,
    out_ref,
    qkv,
    txt,
    hid,
    weights,
    att,
    lhs,
    acc,
    load_sems,
    cw_send,
    cw_recv,
    ccw_send,
    ccw_recv,
    y_send,
    y_recv,
    own_sems,
    part_send,
    part_recv,
):
    windows, tokens, _ = qkv.shape
    text = txt.shape[1]
    rows = wp_hbm.shape[0]
    width = weights.shape[1]
    features = HEADS * HD
    third = width // 3
    half = third // 2
    chips = n // 2
    length = chips // 2
    group = lax.axis_index("group")
    me = lax.axis_index("win")
    core = me % 2
    chip = me // 2
    depth, side = chip // 2, chip % 2
    place = depth + side * (chips - 1 - 2 * depth)

    def chip_at(position):
        spot = (position + chips) % chips
        turn = spot // length
        return 2 * (spot + turn * (chips - 1 - 2 * spot)) + turn

    def ranked(which_chip, which_core):
        return which_chip * 2 + which_core

    onward = (group, ranked(chip_at(place + 1), core))
    backward = (group, ranked(chip_at(place - 1), core))
    across = (1 - group, me)
    partner = (group, me + 1 - 2 * core)
    own_third = group * (2 * third)
    far_third = (1 - group) * (2 * third)

    def region(which_chip, which_core, col, cols):
        row = pl.multiple_of(ranked(which_chip, which_core) * rows, 16)
        return weights.at[pl.ds(row, rows), pl.ds(pl.multiple_of(col, 128), cols)]

    def remote(ref, send, recv, device):
        return pltpu.make_async_remote_copy(
            src_ref=ref, dst_ref=ref, send_sem=send, recv_sem=recv,
            device_id=device, device_id_type=MESH_ID,
        )

    def cw(step, sub, hop):
        ref = region(chip_at(place - step - hop), core, own_third + sub * half, half)
        return remote(ref, cw_send.at[step, sub], cw_recv.at[step, sub], onward)

    def ccw(step, sub, hop):
        ref = region(chip_at(place + step + hop), core, third + sub * half, half)
        return remote(ref, ccw_send.at[step, sub], ccw_recv.at[step, sub], backward)

    def yy(step, sub, col):
        ref = region(chip_at(place - step - 1), core, col + sub * half, half)
        return remote(ref, y_send.at[step, sub], y_recv.at[step, sub], across)

    def part(step, kind, which_core):
        col = (own_third, third, far_third)[kind]
        source = chip_at(place + step + 1) if kind == 1 else chip_at(place - step - 1)
        ref = region(source, which_core, col, third)
        return remote(ref, part_send.at[step, kind], part_recv.at[step, kind], partner)

    def part_own(which_core):
        ref = region(chip, which_core, 0, width)
        return remote(ref, own_sems.at[0], own_sems.at[1], partner)

    own_load = pltpu.make_async_copy(wp_hbm, region(chip, core, 0, width), load_sems.at[0])
    own_load.start()
    loads = []
    for w in range(windows):
        loads.append(
            (
                pltpu.make_async_copy(qkv_hbm.at[w], qkv.at[w], load_sems.at[1 + 2 * w]),
                pltpu.make_async_copy(txt_hbm.at[w], txt.at[w], load_sems.at[2 + 2 * w]),
            )
        )
    hid_load = pltpu.make_async_copy(hid_hbm, hid, load_sems.at[1 + 2 * windows])
    for pair in loads:
        for copy in pair:
            copy.start()
    hid_load.start()

    barrier = pltpu.get_barrier_semaphore()
    for device in (onward, backward, across, partner):
        pl.semaphore_signal(barrier, inc=1, device_id=device, device_id_type=MESH_ID)
    pl.semaphore_wait(barrier, 4)

    own_load.wait()
    for sub in range(2):
        cw(0, sub, 0).start()
        ccw(0, sub, 0).start()
    part_own(core).start()

    scale = LOG2E / math.sqrt(HD)

    def attend(w, h):
        col = pl.multiple_of(h * HD, HD)
        cols = pl.ds(col, HD)
        kcols = pl.ds(pl.multiple_of(col + features, HD), HD)
        vcols = pl.ds(pl.multiple_of(col + 2 * features, HD), HD)
        q = qkv[w, :, cols]
        dims = (((1,), (1,)), ((), ()))
        st = lax.dot_general(txt[w, :, cols], q, dims, preferred_element_type=jnp.float32)
        si = lax.dot_general(qkv[w, :, kcols], q, dims, preferred_element_type=jnp.float32)
        top = jnp.maximum(jnp.max(st, axis=0, keepdims=True), jnp.max(si, axis=0, keepdims=True))
        pt = jnp.exp2((st - top) * scale)
        pi = jnp.exp2((si - top) * scale)
        total = jnp.sum(pt, axis=0, keepdims=True) + jnp.sum(pi, axis=0, keepdims=True)
        back = (((0,), (0,)), ((), ()))
        out = lax.dot_general(
            txt[w, :, kcols], pt.astype(jnp.bfloat16), back, preferred_element_type=jnp.float32
        ) + lax.dot_general(
            qkv[w, :, vcols], pi.astype(jnp.bfloat16), back, preferred_element_type=jnp.float32
        )
        att[pl.ds(col, HD), pl.ds(pl.multiple_of(w * tokens, 128), tokens)] = (
            out * (1.0 / total)
        ).astype(jnp.bfloat16)

    tile = 256 if third % 256 == 0 else third

    def project(left_chip, col, cols, first=False):
        row = pl.multiple_of(left_chip * (2 * rows), 16)
        lhs[...] = att[pl.ds(row, 2 * rows), :].T

        def one(t, carry):
            at = pl.ds(pl.multiple_of(col + t * tile, 128), tile)
            term = jnp.dot(
                lhs[...], weights[pl.ds(row, 2 * rows), at], preferred_element_type=jnp.float32
            )
            acc[:, at] = term if first else acc[:, at] + term
            return carry

        lax.fori_loop(0, cols // tile, one, 0)

    def project_step(step):
        for kind in range(3):
            part(step, kind, 1 - core).wait_recv()
        project(chip_at(place - step - 1), own_third, third)
        project(chip_at(place - step - 1), far_third, third)
        project(chip_at(place + step + 1), third, third)

    def serve(step, sub, more):
        cw(step, sub, 1).wait_recv()
        if more:
            cw(step + 1, sub, 0).start()
        yy(step, sub, own_third).start()
        ccw(step, sub, 1).wait_recv()
        if more:
            ccw(step + 1, sub, 0).start()

    def hand_over(step):
        part(step, 0, core).start()
        part(step, 1, core).start()

    def hand_across(step):
        for sub in range(2):
            yy(step, sub, far_third).wait_recv()
        part(step, 2, core).start()

    steps = chips - 1
    early = (steps + 1) // 2
    slots = 2 * early
    units = windows * HEADS
    per = -(-units // slots)
    done = 0
    plan = []
    for slot in range(slots):
        plan.append(range(done, min(units, done + per)))
        done = min(units, done + per)
    ready = set()
    for step in range(early):
        for sub in range(2):
            for unit in plan[2 * step + sub]:
                w, h = unit // HEADS, unit % HEADS
                if w not in ready:
                    for copy in loads[w]:
                        copy.wait()
                    ready.add(w)
                attend(w, h)
            serve(step, sub, step + 1 < steps)
        hand_over(step)
        if step >= 1:
            hand_across(step - 1)
    part_own(1 - core).wait_recv()
    project(chip, 0, width, first=True)
    due = 0
    for step in range(early, steps):
        for sub in range(2):
            if due <= step - 2:
                project_step(due)
                due += 1
            serve(step, sub, step + 1 < steps)
        hand_over(step)
        hand_across(step - 1)
    hand_across(steps - 1)
    while due < steps:
        project_step(due)
        due += 1

    hid_load.wait()
    block = 64 if acc.shape[0] % 64 == 0 else acc.shape[0]
    gate = mod_ref[0:1, :]
    gain = 1.0 + mod_ref[1:2, :]
    shift = mod_ref[2:3, :]

    def norm(b, carry):
        at = pl.ds(pl.multiple_of(b * block, 16), block)
        residual = hid[at, :].astype(jnp.float32) + gate * acc[at, :]
        mean = jnp.sum(residual, axis=-1, keepdims=True) * (1.0 / width)
        centred = residual - mean
        var = jnp.sum(centred * centred, axis=-1, keepdims=True) * (1.0 / width)
        modulated = (centred * lax.rsqrt(var + 1e-06) * gain + shift).astype(jnp.bfloat16)
        out_ref[at, :] = jnp.dot(modulated, wout_ref[...], preferred_element_type=jnp.float32)
        return carry

    lax.fori_loop(0, acc.shape[0] // block, norm, 0)

    for step in range(steps):
        for sub in range(2):
            cw(step, sub, 0).wait_send()
            ccw(step, sub, 0).wait_send()
            yy(step, sub, own_third).wait_send()
        for kind in range(3):
            part(step, kind, core).wait_send()
    part_own(core).wait_send()


def shards(n, img_qkv, txt_kv, hidden, w_proj, w_out, modulation, anchors, blend_weight):
    windows, tokens, qkv_width = img_qkv.shape
    rows, width = w_proj.shape
    total = windows * tokens
    steps = n // 2 - 1
    any_space = pl.BlockSpec(memory_space=pl.ANY)
    vmem = pl.BlockSpec(memory_space=pltpu.VMEM)
    dma = pltpu.SemaphoreType.DMA
    patch_vel = pl.pallas_call(
        functools.partial(block_kernel, n),
        out_shape=jax.ShapeDtypeStruct((total, w_out.shape[1]), jnp.float32),
        in_specs=[any_space] * 4 + [vmem] * 2,
        out_specs=vmem,
        scratch_shapes=[
            pltpu.VMEM(img_qkv.shape, jnp.bfloat16),
            pltpu.VMEM(txt_kv.shape, jnp.bfloat16),
            pltpu.VMEM((total, width), jnp.bfloat16),
            pltpu.VMEM((n * rows, width), jnp.bfloat16),
            pltpu.VMEM((n * rows, total), jnp.bfloat16),
            pltpu.VMEM((total, 2 * rows), jnp.bfloat16),
            pltpu.VMEM((total, width), jnp.float32),
            dma((2 + 2 * windows,)),
            dma((steps, 2)),
            dma((steps, 2)),
            dma((steps, 2)),
            dma((steps, 2)),
            dma((steps, 2)),
            dma((steps, 2)),
            dma((2,)),
            dma((steps, 3)),
            dma((steps, 3)),
        ],
        compiler_params=pltpu.CompilerParams(
            collective_id=0, has_side_effects=True, vmem_limit_bytes=60 * 1024 * 1024
        ),
    )(img_qkv, txt_kv, hidden.reshape(total, width), w_proj, w_out, modulation)

    weights = blend_weight.astype(jnp.float32)
    grid = patch_vel.reshape(windows, GRID, GRID, C, PATCH, PATCH)
    window_vel = grid.transpose(0, 3, 1, 4, 2, 5).reshape(windows, C, WIN, WIN)
    contrib = jnp.concatenate([window_vel * weights[:, None], weights[:, None]], axis=1)
    band_start = lax.axis_index("win") * BAND
    cells = jnp.arange(WIN, dtype=jnp.int32)
    row_of = anchors[:, 0:1] - band_start + cells
    col_of = (anchors[:, 1:2] + cells) % LW
    row_hot = (row_of[:, :, None] == jnp.arange(BAND + WIN, dtype=jnp.int32)).astype(jnp.float32)
    col_hot = (col_of[:, :, None] == jnp.arange(LW, dtype=jnp.int32)).astype(jnp.float32)
    wide = jnp.einsum("wcab,wbs->wcas", contrib, col_hot, precision=lax.Precision.HIGHEST)
    canvas = jnp.einsum("wcas,war->crs", wide, row_hot, precision=lax.Precision.HIGHEST)
    near = shifted(canvas[:, BAND : 2 * BAND], "win", 1)
    far = shifted(canvas[:, 2 * BAND :], "win", 2)
    summed = canvas[:, :BAND] + near + far
    return summed[:C] / jnp.maximum(summed[C], 1.0)[None]


def solution(mesh):
    in_specs = (
        P(("group", "win"), None, None),
        P(("group", "win"), None, None),
        P(("group", "win"), None, None),
        P("win", None),
        P(),
        P("group", None),
        P(("group", "win"), None),
        P(("group", "win"), None, None),
    )
    out_specs = P(None, ("group", "win"), None)
    n = mesh.shape["win"]

    def body(*args):
        rows, width = args[3].shape
        ringed = mesh.shape["group"] == 2 and n % 4 == 0 and rows % 16 == 0 and width % 768 == 0
        if ringed:
            return shards(n, *args)
        return plain_shards(*args)

    return jax.shard_map(body, mesh=mesh, in_specs=in_specs, out_specs=out_specs, check_vma=False)
```

```python
import functools
import math

import jax
import jax.numpy as jnp
from jax import lax
from jax.experimental import pallas as pl
from jax.experimental.pallas import tpu as pltpu
from jax.sharding import PartitionSpec as P

HD = 128
C = 16
HEADS = 12
PATCH = 2
WIN = 32
LW = 64
BAND = 16
GRID = 16


def shifted(block, axis, distance):
    devices = range(lax.axis_size(axis))
    route = [(i - distance, i) for i in devices if i - distance in devices]
    return lax.ppermute(block, axis, route)


def place_window(canvas, totals, contrib, weights, row_at, col_at):
    zero_index = jnp.zeros((), jnp.int32)
    region = lax.dynamic_slice(canvas, (zero_index, row_at, col_at), (C, WIN, WIN))
    canvas = lax.dynamic_update_slice(canvas, region + contrib, (zero_index, row_at, col_at))
    weight_region = lax.dynamic_slice(totals, (row_at, col_at), (WIN, WIN))
    totals = lax.dynamic_update_slice(totals, weight_region + weights, (row_at, col_at))
    return (canvas, totals)


def fold_columns(field):
    span_cols = field.shape[-1] - WIN
    leading = field[..., :span_cols]
    wrapped = field[..., span_cols:]
    padding = [(0, 0)] * (field.ndim - 1) + [(0, span_cols - WIN)]
    return leading + jnp.pad(wrapped, padding)


def plain_shards(img_qkv, txt_kv, hidden, w_proj, w_out, modulation, anchors, blend_weight):
    window_count, tokens, _ = img_qkv.shape
    features = HEADS * HD
    queries = img_qkv[:, :, :features].reshape(window_count, tokens, HEADS, HD)
    all_keys = jnp.concatenate(
        [txt_kv[:, :, :features], img_qkv[:, :, features : 2 * features]], axis=1
    )
    all_keys = all_keys.reshape(window_count, -1, HEADS, HD)
    all_values = jnp.concatenate([txt_kv[:, :, features:], img_qkv[:, :, 2 * features :]], axis=1)
    all_values = all_values.reshape(window_count, -1, HEADS, HD)
    scores = jnp.einsum(
        "wqhd,wkhd->whqk", queries, all_keys, preferred_element_type=jnp.float32
    ) / math.sqrt(HD)
    scores = scores - jnp.max(scores, axis=-1, keepdims=True)
    exp_scores = jnp.exp(scores)
    soft_weights = (exp_scores / jnp.sum(exp_scores, axis=-1, keepdims=True)).astype(jnp.bfloat16)
    attended = jnp.einsum(
        "whqk,wkhd->wqhd", soft_weights, all_values, preferred_element_type=jnp.float32
    )
    attended = attended.reshape(window_count * tokens, features).astype(jnp.bfloat16)
    whole_proj = lax.all_gather(w_proj, "win", axis=0, tiled=True)
    projected = jnp.dot(attended, whole_proj, preferred_element_type=jnp.float32)
    residual = (
        hidden.reshape(window_count * tokens, -1).astype(jnp.float32) + modulation[0] * projected
    )
    row_mean = jnp.mean(residual, axis=-1, keepdims=True)
    centred = residual - row_mean
    row_var = jnp.mean(centred * centred, axis=-1, keepdims=True)
    normed = centred * lax.rsqrt(row_var + 1e-06)
    modulated = (normed * (1.0 + modulation[1]) + modulation[2]).astype(jnp.bfloat16)
    patch_vel = jnp.dot(modulated, w_out, preferred_element_type=jnp.float32)
    patch_grid = patch_vel.reshape(window_count, GRID, GRID, C, PATCH, PATCH)
    window_vel = patch_grid.transpose(0, 3, 1, 4, 2, 5).reshape(window_count, C, WIN, WIN)
    weights = blend_weight.astype(jnp.float32)
    contrib = window_vel * weights[:, None]
    band_start = lax.axis_index("win") * BAND
    canvas = jnp.zeros((C, BAND + WIN, LW + WIN), jnp.float32)
    totals = jnp.zeros((BAND + WIN, LW + WIN), jnp.float32)

    def add_one(window, running):
        row_at = anchors[window, 0] - band_start
        col_at = anchors[window, 1]
        return place_window(
            running[0], running[1], contrib[window], weights[window], row_at, col_at
        )

    canvas, totals = lax.fori_loop(0, window_count, add_one, (canvas, totals))
    canvas = fold_columns(canvas)
    totals = fold_columns(totals)
    own_canvas = canvas[:, :BAND]
    own_totals = totals[:BAND]
    near_canvas = canvas[:, BAND : 2 * BAND]
    near_totals = totals[BAND : 2 * BAND]
    far_canvas = canvas[:, 2 * BAND :]
    far_totals = totals[2 * BAND :]
    prev_canvas, prev_totals = shifted((near_canvas, near_totals), "win", 1)
    second_canvas, second_totals = shifted((far_canvas, far_totals), "win", 2)
    sum_canvas = own_canvas + prev_canvas + second_canvas
    sum_totals = own_totals + prev_totals + second_totals
    return sum_canvas / jnp.maximum(sum_totals, 1.0)[None]


LOG2E = 1.4426950408889634
MESH_ID = pl.DeviceIdType.MESH


def block_kernel(
    n,
    qkv_hbm,
    txt_hbm,
    hid_hbm,
    wp_hbm,
    wout_ref,
    mod_ref,
    out_ref,
    qkv,
    txt,
    hid,
    weights,
    att,
    lhs,
    acc,
    load_sems,
    cw_send,
    cw_recv,
    ccw_send,
    ccw_recv,
    y_send,
    y_recv,
    own_sems,
    part_send,
    part_recv,
):
    windows, tokens, _ = qkv.shape
    text = txt.shape[1]
    rows = wp_hbm.shape[0]
    width = weights.shape[1]
    features = HEADS * HD
    third = width // 3
    half = third // 2
    chips = n // 2
    length = chips // 2
    group = lax.axis_index("group")
    me = lax.axis_index("win")
    core = me % 2
    chip = me // 2
    depth, side = chip // 2, chip % 2
    place = depth + side * (chips - 1 - 2 * depth)

    def chip_at(position):
        spot = (position + chips) % chips
        turn = spot // length
        return 2 * (spot + turn * (chips - 1 - 2 * spot)) + turn

    def ranked(which_chip, which_core):
        return which_chip * 2 + which_core

    onward = (group, ranked(chip_at(place + 1), core))
    backward = (group, ranked(chip_at(place - 1), core))
    across = (1 - group, me)
    partner = (group, me + 1 - 2 * core)
    own_third = group * (2 * third)
    far_third = (1 - group) * (2 * third)

    def region(which_chip, which_core, col, cols):
        row = pl.multiple_of(ranked(which_chip, which_core) * rows, 16)
        return weights.at[pl.ds(row, rows), pl.ds(pl.multiple_of(col, 128), cols)]

    def remote(ref, send, recv, device):
        return pltpu.make_async_remote_copy(
            src_ref=ref, dst_ref=ref, send_sem=send, recv_sem=recv,
            device_id=device, device_id_type=MESH_ID,
        )

    def cw(step, sub, hop):
        ref = region(chip_at(place - step - hop), core, own_third + sub * half, half)
        return remote(ref, cw_send.at[step, sub], cw_recv.at[step, sub], onward)

    def ccw(step, sub, hop):
        ref = region(chip_at(place + step + hop), core, third + sub * half, half)
        return remote(ref, ccw_send.at[step, sub], ccw_recv.at[step, sub], backward)

    def yy(step, sub, col):
        ref = region(chip_at(place - step - 1), core, col + sub * half, half)
        return remote(ref, y_send.at[step, sub], y_recv.at[step, sub], across)

    def part(step, kind, which_core):
        col = (own_third, third, far_third)[kind]
        source = chip_at(place + step + 1) if kind == 1 else chip_at(place - step - 1)
        ref = region(source, which_core, col, third)
        return remote(ref, part_send.at[step, kind], part_recv.at[step, kind], partner)

    def part_own(which_core):
        ref = region(chip, which_core, 0, width)
        return remote(ref, own_sems.at[0], own_sems.at[1], partner)

    own_load = pltpu.make_async_copy(wp_hbm, region(chip, core, 0, width), load_sems.at[0])
    own_load.start()
    loads = []
    for w in range(windows):
        loads.append(
            (
                pltpu.make_async_copy(qkv_hbm.at[w], qkv.at[w], load_sems.at[1 + 2 * w]),
                pltpu.make_async_copy(txt_hbm.at[w], txt.at[w], load_sems.at[2 + 2 * w]),
            )
        )
    hid_load = pltpu.make_async_copy(hid_hbm, hid, load_sems.at[1 + 2 * windows])

    barrier = pltpu.get_barrier_semaphore()
    for device in (onward, backward, across, partner):
        pl.semaphore_signal(barrier, inc=1, device_id=device, device_id_type=MESH_ID)
    pl.semaphore_wait(barrier, 4)

    own_load.wait()
    for sub in range(2):
        cw(0, sub, 0).start()
        ccw(0, sub, 0).start()
    part_own(core).start()
    for pair in loads:
        for copy in pair:
            copy.start()
    hid_load.start()

    scale = LOG2E / math.sqrt(HD)

    def attend(w, h):
        col = pl.multiple_of(h * HD, HD)
        cols = pl.ds(col, HD)
        kcols = pl.ds(pl.multiple_of(col + features, HD), HD)
        vcols = pl.ds(pl.multiple_of(col + 2 * features, HD), HD)
        q = qkv[w, :, cols]
        dims = (((1,), (1,)), ((), ()))
        st = lax.dot_general(txt[w, :, cols], q, dims, preferred_element_type=jnp.float32)
        si = lax.dot_general(qkv[w, :, kcols], q, dims, preferred_element_type=jnp.float32)
        top = jnp.maximum(jnp.max(st, axis=0, keepdims=True), jnp.max(si, axis=0, keepdims=True))
        pt = jnp.exp2((st - top) * scale)
        pi = jnp.exp2((si - top) * scale)
        total = jnp.sum(pt, axis=0, keepdims=True) + jnp.sum(pi, axis=0, keepdims=True)
        back = (((0,), (0,)), ((), ()))
        out = lax.dot_general(
            txt[w, :, kcols], pt.astype(jnp.bfloat16), back, preferred_element_type=jnp.float32
        ) + lax.dot_general(
            qkv[w, :, vcols], pi.astype(jnp.bfloat16), back, preferred_element_type=jnp.float32
        )
        att[pl.ds(col, HD), pl.ds(pl.multiple_of(w * tokens, 128), tokens)] = (
            out * (1.0 / total)
        ).astype(jnp.bfloat16)

    tile = 512 if third % 512 == 0 else third

    def project(held, col, first=False):
        spots = [pl.ds(pl.multiple_of(q * (2 * rows), 16), 2 * rows) for q in held]
        deep = 2 * rows * len(held)
        lhs[:, :deep] = jnp.concatenate([att[spot, :] for spot in spots], axis=0).T

        def one(t, carry):
            at = pl.ds(pl.multiple_of(col + t * tile, 128), tile)
            rhs = jnp.concatenate([weights[spot, at] for spot in spots], axis=0)
            term = jnp.dot(lhs[:, :deep], rhs, preferred_element_type=jnp.float32)
            acc[:, at] = term if first else acc[:, at] + term
            return carry

        lax.fori_loop(0, third // tile, one, 0)

    def project_kind(group_steps, kind, with_own=False):
        for step in group_steps:
            part(step, kind, 1 - core).wait_recv()
        sign = 1 if kind == 1 else -1
        held = [chip_at(place + sign * (step + 1)) for step in group_steps]
        if with_own:
            held = [chip] + held
        project(held, (own_third, third, far_third)[kind], first=with_own)

    def serve(step, sub, more):
        cw(step, sub, 1).wait_recv()
        if more:
            cw(step + 1, sub, 0).start()
        yy(step, sub, own_third).start()
        ccw(step, sub, 1).wait_recv()
        if more:
            ccw(step + 1, sub, 0).start()

    def hand_over(step):
        part(step, 0, core).start()
        part(step, 1, core).start()

    def hand_across(step):
        for sub in range(2):
            yy(step, sub, far_third).wait_recv()
        part(step, 2, core).start()

    steps = chips - 1
    early = (steps + 1) // 2
    slots = 2 * early
    units = windows * HEADS
    per = -(-units // slots)
    done = 0
    plan = []
    for slot in range(slots):
        plan.append(range(done, min(units, done + per)))
        done = min(units, done + per)
    ready = set()
    for step in range(early):
        for sub in range(2):
            for unit in plan[2 * step + sub]:
                w, h = unit // HEADS, unit % HEADS
                if w not in ready:
                    for copy in loads[w]:
                        copy.wait()
                    ready.add(w)
                attend(w, h)
            serve(step, sub, step + 1 < steps)
        hand_over(step)
        if step >= 1:
            hand_across(step - 1)
    part_own(1 - core).wait_recv()
    opening = list(range(early - 1))
    middle = list(range(early - 1, steps - 2))
    closing = list(range(max(steps - 2, early - 1), steps))
    work = [(opening, kind, True) for kind in (0, 2, 1)]
    work += [None] * (2 * (steps - early) - 5)
    if middle:
        work += [(middle, kind, False) for kind in (0, 2, 1)]
    for step in range(early, steps):
        for sub in range(2):
            quota = 1 if step < steps - 1 else 2
            for _ in range(quota):
                if work:
                    piece = work.pop(0)
                    if piece is not None:
                        project_kind(*piece)
            serve(step, sub, step + 1 < steps)
        hand_over(step)
        hand_across(step - 1)
    for piece in work:
        if piece is not None:
            project_kind(*piece)
    for step in closing[:-1]:
        for kind in range(3):
            project_kind([step], kind)
    hand_across(steps - 1)
    for kind in (0, 1, 2):
        project_kind(closing[-1:], kind)

    hid_load.wait()
    block = 64 if acc.shape[0] % 64 == 0 else acc.shape[0]
    gate = mod_ref[0:1, :]
    gain = 1.0 + mod_ref[1:2, :]
    shift = mod_ref[2:3, :]

    def norm(b, carry):
        at = pl.ds(pl.multiple_of(b * block, 16), block)
        residual = hid[at, :].astype(jnp.float32) + gate * acc[at, :]
        mean = jnp.sum(residual, axis=-1, keepdims=True) * (1.0 / width)
        centred = residual - mean
        var = jnp.sum(centred * centred, axis=-1, keepdims=True) * (1.0 / width)
        modulated = (centred * lax.rsqrt(var + 1e-06) * gain + shift).astype(jnp.bfloat16)
        out_ref[at, :] = lax.dot_general(
            modulated, wout_ref[...], (((1,), (1,)), ((), ())), preferred_element_type=jnp.float32
        )
        return carry

    lax.fori_loop(0, acc.shape[0] // block, norm, 0)

    for step in range(steps):
        for sub in range(2):
            cw(step, sub, 0).wait_send()
            ccw(step, sub, 0).wait_send()
            yy(step, sub, own_third).wait_send()
        for kind in range(3):
            part(step, kind, core).wait_send()
    part_own(core).wait_send()


def shards(n, img_qkv, txt_kv, hidden, w_proj, w_out, modulation, anchors, blend_weight):
    windows, tokens, qkv_width = img_qkv.shape
    rows, width = w_proj.shape
    total = windows * tokens
    steps = n // 2 - 1
    any_space = pl.BlockSpec(memory_space=pl.ANY)
    vmem = pl.BlockSpec(memory_space=pltpu.VMEM)
    dma = pltpu.SemaphoreType.DMA
    patch_vel = pl.pallas_call(
        functools.partial(block_kernel, n),
        out_shape=jax.ShapeDtypeStruct((total, w_out.shape[1]), jnp.float32),
        in_specs=[any_space] * 4 + [vmem] * 2,
        out_specs=vmem,
        scratch_shapes=[
            pltpu.VMEM(img_qkv.shape, jnp.bfloat16),
            pltpu.VMEM(txt_kv.shape, jnp.bfloat16),
            pltpu.VMEM((total, width), jnp.bfloat16),
            pltpu.VMEM((n * rows, width), jnp.bfloat16),
            pltpu.VMEM((n * rows, total), jnp.bfloat16),
            pltpu.VMEM((total, 2 * rows * (n // 4)), jnp.bfloat16),
            pltpu.VMEM((total, width), jnp.float32),
            dma((2 + 2 * windows,)),
            dma((steps, 2)),
            dma((steps, 2)),
            dma((steps, 2)),
            dma((steps, 2)),
            dma((steps, 2)),
            dma((steps, 2)),
            dma((2,)),
            dma((steps, 3)),
            dma((steps, 3)),
        ],
        compiler_params=pltpu.CompilerParams(
            collective_id=0, has_side_effects=True, vmem_limit_bytes=60 * 1024 * 1024
        ),
    )(img_qkv, txt_kv, hidden.reshape(total, width), w_proj, w_out.T, modulation)

    weights = blend_weight.astype(jnp.float32)
    grid = patch_vel.reshape(windows, GRID, GRID, C, PATCH, PATCH)
    window_vel = grid.transpose(0, 3, 1, 4, 2, 5).reshape(windows, C, WIN, WIN)
    contrib = jnp.concatenate([window_vel * weights[:, None], weights[:, None]], axis=1)
    band_start = lax.axis_index("win") * BAND
    cells = jnp.arange(WIN, dtype=jnp.int32)
    row_of = anchors[:, 0:1] - band_start + cells
    col_of = (anchors[:, 1:2] + cells) % LW
    row_hot = (row_of[:, :, None] == jnp.arange(BAND + WIN, dtype=jnp.int32)).astype(jnp.float32)
    col_hot = (col_of[:, :, None] == jnp.arange(LW, dtype=jnp.int32)).astype(jnp.float32)
    wide = jnp.einsum("wcab,wbs->wcas", contrib, col_hot, precision=lax.Precision.HIGHEST)
    canvas = jnp.einsum("wcas,war->crs", wide, row_hot, precision=lax.Precision.HIGHEST)
    near = shifted(canvas[:, BAND : 2 * BAND], "win", 1)
    far = shifted(canvas[:, 2 * BAND :], "win", 2)
    summed = canvas[:, :BAND] + near + far
    return summed[:C] / jnp.maximum(summed[C], 1.0)[None]


def solution(mesh):
    in_specs = (
        P(("group", "win"), None, None),
        P(("group", "win"), None, None),
        P(("group", "win"), None, None),
        P("win", None),
        P(),
        P("group", None),
        P(("group", "win"), None),
        P(("group", "win"), None, None),
    )
    out_specs = P(None, ("group", "win"), None)
    n = mesh.shape["win"]

    def body(*args):
        rows, width = args[3].shape
        ringed = mesh.shape["group"] == 2 and n % 4 == 0 and rows % 16 == 0 and width % 768 == 0
        if ringed:
            return shards(n, *args)
        return plain_shards(*args)

    return jax.shard_map(body, mesh=mesh, in_specs=in_specs, out_specs=out_specs, check_vma=False)
```

```python
import functools
import math

import jax
import jax.numpy as jnp
from jax import lax
from jax.experimental import pallas as pl
from jax.experimental.pallas import tpu as pltpu
from jax.sharding import PartitionSpec as P

HD = 128
C = 16
HEADS = 12
PATCH = 2
WIN = 32
LW = 64
BAND = 16
GRID = 16


def shifted(block, axis, distance):
    devices = range(lax.axis_size(axis))
    route = [(i - distance, i) for i in devices if i - distance in devices]
    return lax.ppermute(block, axis, route)


def place_window(canvas, totals, contrib, weights, row_at, col_at):
    zero_index = jnp.zeros((), jnp.int32)
    region = lax.dynamic_slice(canvas, (zero_index, row_at, col_at), (C, WIN, WIN))
    canvas = lax.dynamic_update_slice(canvas, region + contrib, (zero_index, row_at, col_at))
    weight_region = lax.dynamic_slice(totals, (row_at, col_at), (WIN, WIN))
    totals = lax.dynamic_update_slice(totals, weight_region + weights, (row_at, col_at))
    return (canvas, totals)


def fold_columns(field):
    span_cols = field.shape[-1] - WIN
    leading = field[..., :span_cols]
    wrapped = field[..., span_cols:]
    padding = [(0, 0)] * (field.ndim - 1) + [(0, span_cols - WIN)]
    return leading + jnp.pad(wrapped, padding)


def plain_shards(img_qkv, txt_kv, hidden, w_proj, w_out, modulation, anchors, blend_weight):
    window_count, tokens, _ = img_qkv.shape
    features = HEADS * HD
    queries = img_qkv[:, :, :features].reshape(window_count, tokens, HEADS, HD)
    all_keys = jnp.concatenate(
        [txt_kv[:, :, :features], img_qkv[:, :, features : 2 * features]], axis=1
    )
    all_keys = all_keys.reshape(window_count, -1, HEADS, HD)
    all_values = jnp.concatenate([txt_kv[:, :, features:], img_qkv[:, :, 2 * features :]], axis=1)
    all_values = all_values.reshape(window_count, -1, HEADS, HD)
    scores = jnp.einsum(
        "wqhd,wkhd->whqk", queries, all_keys, preferred_element_type=jnp.float32
    ) / math.sqrt(HD)
    scores = scores - jnp.max(scores, axis=-1, keepdims=True)
    exp_scores = jnp.exp(scores)
    soft_weights = (exp_scores / jnp.sum(exp_scores, axis=-1, keepdims=True)).astype(jnp.bfloat16)
    attended = jnp.einsum(
        "whqk,wkhd->wqhd", soft_weights, all_values, preferred_element_type=jnp.float32
    )
    attended = attended.reshape(window_count * tokens, features).astype(jnp.bfloat16)
    whole_proj = lax.all_gather(w_proj, "win", axis=0, tiled=True)
    projected = jnp.dot(attended, whole_proj, preferred_element_type=jnp.float32)
    residual = (
        hidden.reshape(window_count * tokens, -1).astype(jnp.float32) + modulation[0] * projected
    )
    row_mean = jnp.mean(residual, axis=-1, keepdims=True)
    centred = residual - row_mean
    row_var = jnp.mean(centred * centred, axis=-1, keepdims=True)
    normed = centred * lax.rsqrt(row_var + 1e-06)
    modulated = (normed * (1.0 + modulation[1]) + modulation[2]).astype(jnp.bfloat16)
    patch_vel = jnp.dot(modulated, w_out, preferred_element_type=jnp.float32)
    patch_grid = patch_vel.reshape(window_count, GRID, GRID, C, PATCH, PATCH)
    window_vel = patch_grid.transpose(0, 3, 1, 4, 2, 5).reshape(window_count, C, WIN, WIN)
    weights = blend_weight.astype(jnp.float32)
    contrib = window_vel * weights[:, None]
    band_start = lax.axis_index("win") * BAND
    canvas = jnp.zeros((C, BAND + WIN, LW + WIN), jnp.float32)
    totals = jnp.zeros((BAND + WIN, LW + WIN), jnp.float32)

    def add_one(window, running):
        row_at = anchors[window, 0] - band_start
        col_at = anchors[window, 1]
        return place_window(
            running[0], running[1], contrib[window], weights[window], row_at, col_at
        )

    canvas, totals = lax.fori_loop(0, window_count, add_one, (canvas, totals))
    canvas = fold_columns(canvas)
    totals = fold_columns(totals)
    own_canvas = canvas[:, :BAND]
    own_totals = totals[:BAND]
    near_canvas = canvas[:, BAND : 2 * BAND]
    near_totals = totals[BAND : 2 * BAND]
    far_canvas = canvas[:, 2 * BAND :]
    far_totals = totals[2 * BAND :]
    prev_canvas, prev_totals = shifted((near_canvas, near_totals), "win", 1)
    second_canvas, second_totals = shifted((far_canvas, far_totals), "win", 2)
    sum_canvas = own_canvas + prev_canvas + second_canvas
    sum_totals = own_totals + prev_totals + second_totals
    return sum_canvas / jnp.maximum(sum_totals, 1.0)[None]


LOG2E = 1.4426950408889634
MESH_ID = pl.DeviceIdType.MESH


def block_kernel(
    n,
    qkv_hbm,
    txt_hbm,
    hid_hbm,
    wp_hbm,
    wout_ref,
    mod_ref,
    out_ref,
    qkv,
    txt,
    hid,
    weights,
    att,
    lhs,
    acc,
    load_sems,
    cw_send,
    cw_recv,
    ccw_send,
    ccw_recv,
    y_send,
    y_recv,
    own_sems,
    part_send,
    part_recv,
):
    windows, tokens, _ = qkv.shape
    text = txt.shape[1]
    rows = wp_hbm.shape[0]
    width = weights.shape[1]
    features = HEADS * HD
    third = width // 3
    half = third // 2
    chips = n // 2
    length = chips // 2
    group = lax.axis_index("group")
    me = lax.axis_index("win")
    core = me % 2
    chip = me // 2
    depth, side = chip // 2, chip % 2
    place = depth + side * (chips - 1 - 2 * depth)

    def chip_at(position):
        spot = (position + chips) % chips
        turn = spot // length
        return 2 * (spot + turn * (chips - 1 - 2 * spot)) + turn

    def ranked(which_chip, which_core):
        return which_chip * 2 + which_core

    onward = (group, ranked(chip_at(place + 1), core))
    backward = (group, ranked(chip_at(place - 1), core))
    across = (1 - group, me)
    partner = (group, me + 1 - 2 * core)
    own_third = group * (2 * third)
    far_third = (1 - group) * (2 * third)

    def region(which_chip, which_core, col, cols):
        row = pl.multiple_of(ranked(which_chip, which_core) * rows, 16)
        return weights.at[pl.ds(row, rows), pl.ds(pl.multiple_of(col, 128), cols)]

    def remote(ref, send, recv, device):
        return pltpu.make_async_remote_copy(
            src_ref=ref, dst_ref=ref, send_sem=send, recv_sem=recv,
            device_id=device, device_id_type=MESH_ID,
        )

    def cw(step, sub, hop):
        ref = region(chip_at(place - step - hop), core, own_third + sub * half, half)
        return remote(ref, cw_send.at[step, sub], cw_recv.at[step, sub], onward)

    def ccw(step, sub, hop):
        ref = region(chip_at(place + step + hop), core, third + sub * half, half)
        return remote(ref, ccw_send.at[step, sub], ccw_recv.at[step, sub], backward)

    def yy(step, sub, col):
        ref = region(chip_at(place - step - 1), core, col + sub * half, half)
        return remote(ref, y_send.at[step, sub], y_recv.at[step, sub], across)

    def part(step, kind, which_core):
        col = (own_third, third, far_third)[kind]
        source = chip_at(place + step + 1) if kind == 1 else chip_at(place - step - 1)
        ref = region(source, which_core, col, third)
        return remote(ref, part_send.at[step, kind], part_recv.at[step, kind], partner)

    def part_own(which_core):
        ref = region(chip, which_core, 0, width)
        return remote(ref, own_sems.at[0], own_sems.at[1], partner)

    own_load = pltpu.make_async_copy(wp_hbm, region(chip, core, 0, width), load_sems.at[0])
    own_load.start()
    loads = []
    for w in range(windows):
        loads.append(
            (
                pltpu.make_async_copy(qkv_hbm.at[w], qkv.at[w], load_sems.at[1 + 2 * w]),
                pltpu.make_async_copy(txt_hbm.at[w], txt.at[w], load_sems.at[2 + 2 * w]),
            )
        )
    hid_load = pltpu.make_async_copy(hid_hbm, hid, load_sems.at[1 + 2 * windows])

    barrier = pltpu.get_barrier_semaphore()
    for device in (onward, backward, across, partner):
        pl.semaphore_signal(barrier, inc=1, device_id=device, device_id_type=MESH_ID)
    pl.semaphore_wait(barrier, 4)

    own_load.wait()
    for sub in range(2):
        cw(0, sub, 0).start()
        ccw(0, sub, 0).start()
    part_own(core).start()
    for pair in loads:
        for copy in pair:
            copy.start()
    hid_load.start()

    scale = LOG2E / math.sqrt(HD)

    def attend(w, h):
        col = pl.multiple_of(h * HD, HD)
        cols = pl.ds(col, HD)
        kcols = pl.ds(pl.multiple_of(col + features, HD), HD)
        vcols = pl.ds(pl.multiple_of(col + 2 * features, HD), HD)
        q = qkv[w, :, cols]
        dims = (((1,), (1,)), ((), ()))
        st = lax.dot_general(txt[w, :, cols], q, dims, preferred_element_type=jnp.float32)
        si = lax.dot_general(qkv[w, :, kcols], q, dims, preferred_element_type=jnp.float32)
        top = jnp.maximum(jnp.max(st, axis=0, keepdims=True), jnp.max(si, axis=0, keepdims=True))
        pt = jnp.exp2((st - top) * scale)
        pi = jnp.exp2((si - top) * scale)
        total = jnp.sum(pt, axis=0, keepdims=True) + jnp.sum(pi, axis=0, keepdims=True)
        back = (((0,), (0,)), ((), ()))
        out = lax.dot_general(
            txt[w, :, kcols], pt.astype(jnp.bfloat16), back, preferred_element_type=jnp.float32
        ) + lax.dot_general(
            qkv[w, :, vcols], pi.astype(jnp.bfloat16), back, preferred_element_type=jnp.float32
        )
        att[pl.ds(col, HD), pl.ds(pl.multiple_of(w * tokens, 128), tokens)] = (
            out * (1.0 / total)
        ).astype(jnp.bfloat16)

    tile = 512 if third % 512 == 0 else third

    def project(held, col, first=False):
        spots = [pl.ds(pl.multiple_of(q * (2 * rows), 16), 2 * rows) for q in held]
        deep = 2 * rows * len(held)
        lhs[:, :deep] = jnp.concatenate([att[spot, :] for spot in spots], axis=0).T

        def one(t, carry):
            at = pl.ds(pl.multiple_of(col + t * tile, 128), tile)
            rhs = jnp.concatenate([weights[spot, at] for spot in spots], axis=0)
            term = jnp.dot(lhs[:, :deep], rhs, preferred_element_type=jnp.float32)
            acc[:, at] = term if first else acc[:, at] + term
            return carry

        lax.fori_loop(0, third // tile, one, 0)

    def project_kind(group_steps, kind, with_own=False):
        for step in group_steps:
            part(step, kind, 1 - core).wait_recv()
        sign = 1 if kind == 1 else -1
        held = [chip_at(place + sign * (step + 1)) for step in group_steps]
        if with_own:
            held = [chip] + held
        project(held, (own_third, third, far_third)[kind], first=with_own)

    def serve(step, sub, more):
        cw(step, sub, 1).wait_recv()
        if more:
            cw(step + 1, sub, 0).start()
        yy(step, sub, own_third).start()
        ccw(step, sub, 1).wait_recv()
        if more:
            ccw(step + 1, sub, 0).start()

    def hand_over(step):
        part(step, 0, core).start()
        part(step, 1, core).start()

    def hand_across(step):
        for sub in range(2):
            yy(step, sub, far_third).wait_recv()
        part(step, 2, core).start()

    steps = chips - 1
    early = (steps + 1) // 2
    slots = 2 * early
    units = windows * HEADS
    per = -(-units // slots)
    done = 0
    plan = []
    for slot in range(slots):
        plan.append(range(done, min(units, done + per)))
        done = min(units, done + per)
    ready = set()
    for step in range(early):
        for sub in range(2):
            for unit in plan[2 * step + sub]:
                w, h = unit // HEADS, unit % HEADS
                if w not in ready:
                    for copy in loads[w]:
                        copy.wait()
                    ready.add(w)
                attend(w, h)
            serve(step, sub, step + 1 < steps)
        hand_over(step)
        if step >= 1:
            hand_across(step - 1)
    part_own(1 - core).wait_recv()
    opening = list(range(early - 1))
    middle = list(range(early - 1, steps - 2))
    closing = list(range(max(steps - 2, early - 1), steps))
    work = [(opening, kind, True) for kind in (0, 2, 1)]
    work += [None] * (2 * (steps - early) - 5)
    if middle:
        work += [(middle, kind, False) for kind in (0, 2, 1)]
    for step in range(early, steps):
        for sub in range(2):
            quota = 1 if step < steps - 1 else 2
            for _ in range(quota):
                if work:
                    piece = work.pop(0)
                    if piece is not None:
                        project_kind(*piece)
            serve(step, sub, step + 1 < steps)
        hand_over(step)
        hand_across(step - 1)
    for piece in work:
        if piece is not None:
            project_kind(*piece)
    for step in closing[:-1]:
        for kind in range(3):
            project_kind([step], kind)
    hand_across(steps - 1)
    for kind in (0, 1, 2):
        project_kind(closing[-1:], kind)

    hid_load.wait()
    block = 256 if acc.shape[0] % 256 == 0 else acc.shape[0]
    gate = mod_ref[0:1, :]
    gain = 1.0 + mod_ref[1:2, :]
    shift = mod_ref[2:3, :]

    def norm(b, carry):
        at = pl.ds(pl.multiple_of(b * block, 16), block)
        residual = hid[at, :].astype(jnp.float32) + gate * acc[at, :]
        mean = jnp.sum(residual, axis=-1, keepdims=True) * (1.0 / width)
        centred = residual - mean
        var = jnp.sum(centred * centred, axis=-1, keepdims=True) * (1.0 / width)
        modulated = (centred * lax.rsqrt(var + 1e-06) * gain + shift).astype(jnp.bfloat16)
        out_ref[:, pl.ds(pl.multiple_of(b * block, 128), block)] = lax.dot_general(
            wout_ref[...], modulated, (((1,), (1,)), ((), ())), preferred_element_type=jnp.float32
        )
        return carry

    lax.fori_loop(0, acc.shape[0] // block, norm, 0)

    for step in range(steps):
        for sub in range(2):
            cw(step, sub, 0).wait_send()
            ccw(step, sub, 0).wait_send()
            yy(step, sub, own_third).wait_send()
        for kind in range(3):
            part(step, kind, core).wait_send()
    part_own(core).wait_send()


def shards(n, img_qkv, txt_kv, hidden, w_proj, w_out, modulation, anchors, blend_weight):
    windows, tokens, qkv_width = img_qkv.shape
    rows, width = w_proj.shape
    total = windows * tokens
    steps = n // 2 - 1
    any_space = pl.BlockSpec(memory_space=pl.ANY)
    vmem = pl.BlockSpec(memory_space=pltpu.VMEM)
    dma = pltpu.SemaphoreType.DMA
    patch_vel = pl.pallas_call(
        functools.partial(block_kernel, n),
        out_shape=jax.ShapeDtypeStruct((w_out.shape[1], total), jnp.float32),
        in_specs=[any_space] * 4 + [vmem] * 2,
        out_specs=vmem,
        scratch_shapes=[
            pltpu.VMEM(img_qkv.shape, jnp.bfloat16),
            pltpu.VMEM(txt_kv.shape, jnp.bfloat16),
            pltpu.VMEM((total, width), jnp.bfloat16),
            pltpu.VMEM((n * rows, width), jnp.bfloat16),
            pltpu.VMEM((n * rows, total), jnp.bfloat16),
            pltpu.VMEM((total, 2 * rows * (n // 4)), jnp.bfloat16),
            pltpu.VMEM((total, width), jnp.float32),
            dma((2 + 2 * windows,)),
            dma((steps, 2)),
            dma((steps, 2)),
            dma((steps, 2)),
            dma((steps, 2)),
            dma((steps, 2)),
            dma((steps, 2)),
            dma((2,)),
            dma((steps, 3)),
            dma((steps, 3)),
        ],
        compiler_params=pltpu.CompilerParams(
            collective_id=0, has_side_effects=True, vmem_limit_bytes=60 * 1024 * 1024
        ),
    )(img_qkv, txt_kv, hidden.reshape(total, width), w_proj, w_out.T, modulation)

    weights = blend_weight.astype(jnp.float32)
    grid = patch_vel.reshape(C, PATCH, PATCH, windows, GRID, GRID)
    window_vel = grid.transpose(3, 0, 4, 1, 5, 2).reshape(windows, C, WIN, WIN)
    contrib = jnp.concatenate([window_vel * weights[:, None], weights[:, None]], axis=1)
    band_start = lax.axis_index("win") * BAND
    cells = jnp.arange(WIN, dtype=jnp.int32)
    row_of = anchors[:, 0:1] - band_start + cells
    col_of = (anchors[:, 1:2] + cells) % LW
    row_hot = (row_of[:, :, None] == jnp.arange(BAND + WIN, dtype=jnp.int32)).astype(jnp.float32)
    col_hot = (col_of[:, :, None] == jnp.arange(LW, dtype=jnp.int32)).astype(jnp.float32)
    wide = jnp.einsum("wcab,wbs->wcas", contrib, col_hot, precision=lax.Precision.HIGHEST)
    canvas = jnp.einsum("wcas,war->crs", wide, row_hot, precision=lax.Precision.HIGHEST)
    near = shifted(canvas[:, BAND : 2 * BAND], "win", 1)
    far = shifted(canvas[:, 2 * BAND :], "win", 2)
    summed = canvas[:, :BAND] + near + far
    return summed[:C] / jnp.maximum(summed[C], 1.0)[None]


def solution(mesh):
    in_specs = (
        P(("group", "win"), None, None),
        P(("group", "win"), None, None),
        P(("group", "win"), None, None),
        P("win", None),
        P(),
        P("group", None),
        P(("group", "win"), None),
        P(("group", "win"), None, None),
    )
    out_specs = P(None, ("group", "win"), None)
    n = mesh.shape["win"]

    def body(*args):
        rows, width = args[3].shape
        ringed = mesh.shape["group"] == 2 and n % 4 == 0 and rows % 16 == 0 and width % 768 == 0
        if ringed:
            return shards(n, *args)
        return plain_shards(*args)

    return jax.shard_map(body, mesh=mesh, in_specs=in_specs, out_specs=out_specs, check_vma=False)
```
